32 devices in a mesh: cell: 8 (over z, x), grp: 4 (over y, core).
Axes of the slice: x: 2, y: 2, z: 4, core: 2. Of those that a mesh axis runs over, the one named last changes fastest.
Arguments:
- atom_sites: float32 [3, 16384], P(None, ('cell', 'grp')), may hold values from 0 to 8, as said below
- grid_points: float32 [3, 12288], P(None, ('cell', 'grp')), may hold values from 0 to 8, as said below
- dipole_guess: float32 [3, 16384], P(None, ('cell', 'grp')), may hold values from -2 to 2
- fixed_field: float32 [3, 16384], P(None, ('cell', 'grp')), may hold values from -1800 to 1800
- polarisability: float32 [16384], P(('cell', 'grp')), may hold values from 0.0005 to 0.002
- base_charge: float32 [12288], P(('cell', 'grp')), may hold values from -12 to 12
- response: float32 [12288], P(('cell', 'grp')), may hold values from 0.02 to 0.2
- near_blocks: int32 [128, 8], P(('cell', 'grp')), may hold values from 0 to 47, as said below
- grid_blocks: int32 [128, 4], P(('cell', 'grp')), may hold values from 0 to 35, as said below
- source_blocks: int32 [96, 8], P(('cell', 'grp')), may hold values from 0 to 47, as said below
Outputs:
- dipoles: float32 [3, 16384], P(None, ('cell', 'grp'))
- qm_charges: float32 [12288], P(('cell', 'grp'))
The draws below stay inside these ranges and needn't reach their ends.
Inputs may be any that keep to these rules, and one draw needn't show every extreme that they name: `atom_sites`: atom a has first coordinate in [c, c + 1) with c = a // 2048, the other two in [0, 1). `grid_points`: grid point g has first coordinate in [c, c + 1) with c = g // 1536, the other two in [0, 1). `near_blocks`: each row holds 8 distinct MM window indices, never the block's own index 16 + b % 16. `grid_blocks`: each row holds 4 distinct grid window indices. `source_blocks`: each row holds 8 distinct MM window indices.
All inputs are finite; a program needn't handle non-finite values.
Results may differ from the reference program's by a relative error of at most 0.0003.
Values sent between devices are 32-bit elements; how exact they have to be, the bound alone decides.
A program may use at most 64 MiB of HBM per device.

```python
import math
import jax
import jax.numpy as jnp
from jax import lax

BLOCK = 128
NB = 8
NQ = 4
NM = 8
ITERS = 3
CELLS = 8
CELL_BLK = 16
CELL_GBLK = 12
CELL_ATOMS = 2048
CELL_GRID = 1536
BLOCKS = 128
GBLOCKS = 96
ATOMS = 16384
GRID = 12288


def place_points(key, per_cell):
    uniform_unit = jax.random.uniform(key, (3, CELLS * per_cell), jnp.float32)
    shift_x = (jnp.arange(CELLS * per_cell, dtype=jnp.int32) // per_cell).astype(jnp.float32)
    return jnp.stack([uniform_unit[0] + shift_x, uniform_unit[1], uniform_unit[2]])


def window_lists(key, row_count, span, picks, cell_rows, exclude_own):
    scores = jax.random.randint(key, (row_count, span), 0, 1 << 20, dtype=jnp.int32) * span
    scores = scores + jnp.arange(span, dtype=jnp.int32)[None, :]
    if exclude_own:
        own_rows = cell_rows + jnp.arange(row_count, dtype=jnp.int32) % cell_rows
        scores = jnp.where(jnp.arange(span, dtype=jnp.int32)[None, :] == own_rows[:, None], -1, scores)
    return lax.top_k(scores, picks)[1].astype(jnp.int32)


def draw_atom_sites(key, part):
    return place_points(jax.random.fold_in(key, 11), CELL_ATOMS)


def draw_grid_points(key, part):
    return place_points(jax.random.fold_in(key, 12), CELL_GRID)


def draw_near_blocks(key, part):
    return window_lists(jax.random.fold_in(key, 21), BLOCKS, 3 * CELL_BLK, NB, CELL_BLK, True)


def draw_grid_blocks(key, part):
    return window_lists(jax.random.fold_in(key, 22), BLOCKS, 3 * CELL_GBLK, NQ, CELL_GBLK, False)


def draw_source_blocks(key, part):
    return window_lists(jax.random.fold_in(key, 23), GBLOCKS, 3 * CELL_BLK, NM, CELL_BLK, False)


def level_of(own_key, dims, shards, low, top_value):
    def one(dim, blocks):
        steps = jax.random.uniform(jax.random.fold_in(jax.random.fold_in(own_key, 6), dim), (blocks,), jnp.float32, low / len(shards), top_value / len(shards))
        return jnp.repeat(jnp.exp(steps), dims[dim] // blocks).reshape((-1,) + (1,) * (len(dims) - dim - 1))

    gain = one(*shards[0])
    for cut in shards[1:]:
        gain = gain * one(*cut)
    return gain


def scatter_about(own_key, extent, deviation, bound, shards=(), kind=jnp.bfloat16):
    gain = level_of(own_key, extent, shards, -0.22, 0.18) if shards else 1.0
    values = jax.random.normal(own_key, extent, jnp.float32) * deviation * gain
    return jnp.minimum(jnp.maximum(values, -bound), bound).astype(kind)


def setup_inputs(seed: int = 0) -> dict:
    arg_keys = jax.random.split(jax.random.key(seed), 11)
    atom_sites = draw_atom_sites(jax.random.fold_in(arg_keys[10], 71), 0)
    grid_points = draw_grid_points(jax.random.fold_in(arg_keys[10], 71), 0)
    dipole_guess = scatter_about(arg_keys[2], (3, ATOMS), 0.3, 2.0, ((1, 32),), jnp.float32)
    fixed_field = scatter_about(arg_keys[3], (3, ATOMS), 300.0, 1800.0, ((1, 32),), jnp.float32)
    polarisability = jnp.clip(jnp.exp(math.log(0.002) - 1.3862944 * jax.random.uniform(arg_keys[4], (ATOMS,), jnp.float32) ** level_of(arg_keys[4], (ATOMS,), ((0, 32),), -0.2, 0.2)), 0.0005, 0.002)
    base_charge = scatter_about(arg_keys[5], (GRID,), 2.0, 12.0, ((0, 32),), jnp.float32)
    response = jnp.clip(jnp.exp(math.log(0.2) - 2.3025851 * jax.random.uniform(arg_keys[6], (GRID,), jnp.float32) ** level_of(arg_keys[6], (GRID,), ((0, 32),), -0.2, 0.2)), 0.02, 0.2)
    near_blocks = draw_near_blocks(jax.random.fold_in(arg_keys[10], 71), 0)
    grid_blocks = draw_grid_blocks(jax.random.fold_in(arg_keys[10], 71), 0)
    source_blocks = draw_source_blocks(jax.random.fold_in(arg_keys[10], 71), 0)
    return dict(atom_sites=atom_sites, grid_points=grid_points, dipole_guess=dipole_guess, fixed_field=fixed_field, polarisability=polarisability, base_charge=base_charge, response=response, near_blocks=near_blocks, grid_blocks=grid_blocks, source_blocks=source_blocks)


soften_sq = 0.04

def pick_tile(tile_set, slot_index):
    return lax.dynamic_index_in_dim(tile_set, slot_index, 1, keepdims=False)

def pair_geometry(targets, sources):
    delta_x = targets[0][:, None] - sources[0][None, :]
    delta_y = targets[1][:, None] - sources[1][None, :]
    delta_z = targets[2][:, None] - sources[2][None, :]
    inverse = 1.0 / jnp.sqrt(delta_x * delta_x + delta_y * delta_y + delta_z * delta_z + soften_sq)
    inv_cube = inverse * inverse * inverse
    return (delta_x, delta_y, delta_z, inv_cube, inv_cube * inverse * inverse)

def dipole_field(targets, sources, moments, keep_mask):
    delta_x, delta_y, delta_z, inv_cube, inv_fifth = pair_geometry(targets, sources)
    projected = moments[0][None, :] * delta_x + moments[1][None, :] * delta_y + moments[2][None, :] * delta_z
    radial = 3.0 * projected * inv_fifth * keep_mask
    direct = inv_cube * keep_mask
    return jnp.stack([lax.optimization_barrier(jnp.sum(radial * delta_x - moments[0][None, :] * direct, axis=1)), lax.optimization_barrier(jnp.sum(radial * delta_y - moments[1][None, :] * direct, axis=1)), lax.optimization_barrier(jnp.sum(radial * delta_z - moments[2][None, :] * direct, axis=1))])

def charge_field(targets, sources, charges):
    delta_x, delta_y, delta_z, inv_cube, inv_fifth = pair_geometry(targets, sources)
    weight = charges[None, :] * inv_cube
    return jnp.stack([lax.optimization_barrier(jnp.sum(weight * delta_x, axis=1)), lax.optimization_barrier(jnp.sum(weight * delta_y, axis=1)), lax.optimization_barrier(jnp.sum(weight * delta_z, axis=1))])

def dipole_potential(targets, sources, moments):
    delta_x, delta_y, delta_z, inv_cube, inv_fifth = pair_geometry(targets, sources)
    projected = moments[0][None, :] * delta_x + moments[1][None, :] * delta_y + moments[2][None, :] * delta_z
    return lax.optimization_barrier(jnp.sum(projected * inv_cube, axis=1))

def far_geometry(targets, cell_here, cell_count):
    centres = jnp.arange(cell_count, dtype=jnp.int32).astype(jnp.float32) + 0.5
    delta_x = targets[0][None, :] - centres[:, None]
    delta_y = targets[1][None, :] - 0.5
    delta_z = targets[2][None, :] - 0.5
    far_mask = (jnp.abs(jnp.arange(cell_count, dtype=jnp.int32) - cell_here) >= 2).astype(jnp.float32)[:, None]
    inverse = 1.0 / jnp.sqrt(delta_x * delta_x + delta_y * delta_y + delta_z * delta_z + soften_sq)
    inv_cube = inverse * inverse * inverse * far_mask
    return (delta_x, delta_y, delta_z, inv_cube, inv_cube * inverse * inverse)

def far_field(targets, cell_here, moments, charges):
    delta_x, delta_y, delta_z, inv_cube, inv_fifth = far_geometry(targets, cell_here, charges.shape[0])
    projected = moments[:, 0:1] * delta_x + moments[:, 1:2] * delta_y + moments[:, 2:3] * delta_z
    radial = 3.0 * projected * inv_fifth
    coulomb = charges[:, None] * inv_cube
    return jnp.stack([lax.optimization_barrier(jnp.sum(radial * delta_x - moments[:, 0:1] * inv_cube + coulomb * delta_x, axis=0)), lax.optimization_barrier(jnp.sum(radial * delta_y - moments[:, 1:2] * inv_cube + coulomb * delta_y, axis=0)), lax.optimization_barrier(jnp.sum(radial * delta_z - moments[:, 2:3] * inv_cube + coulomb * delta_z, axis=0))])

def far_potential(targets, cell_here, moments):
    delta_x, delta_y, delta_z, inv_cube, inv_fifth = far_geometry(targets, cell_here, moments.shape[0])
    projected = moments[:, 0:1] * delta_x + moments[:, 1:2] * delta_y + moments[:, 2:3] * delta_z
    return lax.optimization_barrier(jnp.sum(projected * inv_cube, axis=0))

def atom_block(targets, own_slot, near_list, grid_list, site_tiles, dipole_tiles, point_tiles, charge_tiles, cell_here, moments, charge_sums):
    tile_width = targets.shape[1]
    self_mask = 1.0 - jnp.eye(tile_width, dtype=jnp.float32)
    accumulated = dipole_field(targets, pick_tile(site_tiles, own_slot), pick_tile(dipole_tiles, own_slot), self_mask)

    def near_step(member, carried):
        other_slot = near_list[member]
        return carried + dipole_field(targets, pick_tile(site_tiles, other_slot), pick_tile(dipole_tiles, other_slot), 1.0)
    accumulated = lax.fori_loop(0, near_list.shape[0], near_step, accumulated)

    def grid_step(member, carried):
        other_slot = grid_list[member]
        return carried + charge_field(targets, pick_tile(point_tiles, other_slot), lax.dynamic_index_in_dim(charge_tiles, other_slot, 0, keepdims=False))
    accumulated = lax.fori_loop(0, grid_list.shape[0], grid_step, accumulated)
    return accumulated + far_field(targets, cell_here, moments, charge_sums)

def grid_block(targets, source_list, site_tiles, dipole_tiles, cell_here, dipole_sums):

    def near_step(member, carried):
        other_slot = source_list[member]
        return carried + dipole_potential(targets, pick_tile(site_tiles, other_slot), pick_tile(dipole_tiles, other_slot))
    accumulated = lax.fori_loop(0, source_list.shape[0], near_step, jnp.zeros((targets.shape[1],), jnp.float32))
    return accumulated + far_potential(targets, cell_here, dipole_sums)

def cell_table(dipoles, charges, grid_points):
    dipole_sums = lax.optimization_barrier(jnp.sum(dipoles.reshape(3, CELLS, CELL_ATOMS), axis=2)).T
    charge_cells = charges.reshape(CELLS, CELL_GRID)
    centres = jnp.stack([jnp.arange(CELLS, dtype=jnp.int32).astype(jnp.float32) + 0.5, jnp.full((CELLS,), 0.5, jnp.float32), jnp.full((CELLS,), 0.5, jnp.float32)])
    offsets = grid_points.reshape(3, CELLS, CELL_GRID) - centres[:, :, None]
    charge_sums = lax.optimization_barrier(jnp.sum(charge_cells, axis=1))
    grid_moments = lax.optimization_barrier(jnp.sum(charge_cells[None, :, :] * offsets, axis=2)).T
    return (dipole_sums, charge_sums, grid_moments)

def reference(atom_sites, grid_points, dipole_guess, fixed_field, polarisability, base_charge, response, near_blocks, grid_blocks, source_blocks):
    target_tiles = atom_sites.reshape(3, BLOCKS, BLOCK)
    grid_targets = grid_points.reshape(3, GBLOCKS, BLOCK)
    site_tiles = jnp.pad(target_tiles, ((0, 0), (CELL_BLK, CELL_BLK), (0, 0)))
    point_tiles = jnp.pad(grid_targets, ((0, 0), (CELL_GBLK, CELL_GBLK), (0, 0)))
    dipoles = dipole_guess
    charges = base_charge
    for iteration in range(ITERS):
        dipole_sums, charge_sums, grid_moments = cell_table(dipoles, charges, grid_points)
        moments = dipole_sums + grid_moments
        dipole_tiles = jnp.pad(dipoles.reshape(3, BLOCKS, BLOCK), ((0, 0), (CELL_BLK, CELL_BLK), (0, 0)))
        charge_tiles = jnp.pad(charges.reshape(GBLOCKS, BLOCK), ((CELL_GBLK, CELL_GBLK), (0, 0)))

        def one_atom_block(block_index):
            cell_here = block_index // CELL_BLK
            window_start = cell_here * CELL_BLK
            grid_start = cell_here * CELL_GBLK
            return atom_block(pick_tile(target_tiles, block_index), block_index - window_start + CELL_BLK, near_blocks[block_index], grid_blocks[block_index], lax.dynamic_slice_in_dim(site_tiles, window_start, 3 * CELL_BLK, 1), lax.dynamic_slice_in_dim(dipole_tiles, window_start, 3 * CELL_BLK, 1), lax.dynamic_slice_in_dim(point_tiles, grid_start, 3 * CELL_GBLK, 1), lax.dynamic_slice_in_dim(charge_tiles, grid_start, 3 * CELL_GBLK, 0), cell_here, moments, charge_sums)

        def one_grid_block(block_index):
            cell_here = block_index // CELL_GBLK
            window_start = cell_here * CELL_BLK
            return grid_block(pick_tile(grid_targets, block_index), source_blocks[block_index], lax.dynamic_slice_in_dim(site_tiles, window_start, 3 * CELL_BLK, 1), lax.dynamic_slice_in_dim(dipole_tiles, window_start, 3 * CELL_BLK, 1), cell_here, dipole_sums)
        induced_field = lax.map(one_atom_block, jnp.arange(BLOCKS, dtype=jnp.int32))
        induced_field = jnp.transpose(induced_field, (1, 0, 2)).reshape(3, ATOMS)
        potential = lax.map(one_grid_block, jnp.arange(GBLOCKS, dtype=jnp.int32)).reshape(GRID)
        dipoles = polarisability[None, :] * (fixed_field + induced_field)
        charges = base_charge - response * potential
    return (dipoles, charges)
```

```python
import functools
import math

import jax
import jax.numpy as jnp
from jax import lax
from jax.experimental import pallas as pl
from jax.experimental.pallas import tpu as pltpu
from jax.sharding import PartitionSpec as P

BLOCK = 128
SUB = 8
GROUPS = BLOCK // SUB
UNROLL = 8
HALVES = GROUPS // UNROLL
ITERS = 3
MESH = pl.DeviceIdType.MESH

soften_sq = 0.04


def round_up(n, m):
    return (n + m - 1) // m * m


def body(dims, *refs):
    cells, grps, na, ng, nb, nq, nm = dims
    near_s, grid_s, source_s, sites, points, guess, fixed, pol, base, resp = refs[:10]
    out_dip, out_q = refs[10:12]
    stat = refs[12]
    dyn = refs[13 : 13 + ITERS]
    tab = refs[13 + ITERS : 13 + 2 * ITERS]
    rest = refs[13 + 2 * ITERS :]
    tgt_a, tgt_g, geo, cgeo, pgeo, fld = rest[:6]
    stat_send, stat_recv, dyn_send, dyn_recv, far_send, far_recv = rest[6:]
    cell = lax.axis_index("cell")
    grp = lax.axis_index("grp")
    has_prev = cell > 0
    has_next = cell < cells - 1
    nk = nb + 1
    own = grps + grp
    cell_f = cell.astype(jnp.float32)
    centre = (cell_f + 0.5, 0.5, 0.5)

    def vec_row(ref, a, b):
        return ref[a : a + 1, b * BLOCK : (b + 1) * BLOCK]

    def flat_row(ref, b):
        return ref[b * BLOCK : (b + 1) * BLOCK].reshape(1, BLOCK)

    lanes = lax.broadcasted_iota(jnp.int32, (SUB, BLOCK), 1)
    subs = lax.broadcasted_iota(jnp.int32, (SUB, BLOCK), 0)
    diag = lanes - subs

    for it in range(ITERS):
        tab[it][...] = jnp.zeros_like(tab[it])

    @pl.when(jnp.logical_not(has_prev))
    def _():
        for p in range(grps):
            stat[p] = jnp.zeros(stat.shape[1:], jnp.float32)
            for it in range(ITERS):
                dyn[it][p] = jnp.zeros(dyn[it].shape[1:], jnp.float32)

    @pl.when(jnp.logical_not(has_next))
    def _():
        for p in range(2 * grps, 3 * grps):
            stat[p] = jnp.zeros(stat.shape[1:], jnp.float32)
            for it in range(ITERS):
                dyn[it][p] = jnp.zeros(dyn[it].shape[1:], jnp.float32)

    barrier = pltpu.get_barrier_semaphore()

    def greet(c, g):
        pl.semaphore_signal(barrier, inc=1, device_id=(c, g), device_id_type=MESH)

    def each_far(act):
        def step(c, carry):
            @pl.when(jnp.abs(c - cell) >= 2)
            def _():
                act(c)

            return carry

        lax.fori_loop(0, cells, step, 0)

    each_far(lambda c: greet(c, grp))

    @pl.when(has_prev)
    def _():
        for j in range(grps):
            greet(cell - 1, j)

    @pl.when(has_next)
    def _():
        for j in range(grps):
            greet(cell + 1, j)

    for d in range(1, grps):
        greet(cell, lax.rem(grp + d, grps))

    for a in range(3):
        for b in range(na):
            stat[own, a * na + b : a * na + b + 1, :] = vec_row(sites, a, b)
            dyn[0][own, a * na + b : a * na + b + 1, :] = vec_row(guess, a, b)
        for b in range(ng):
            r = 3 * na + a * ng + b
            stat[own, r : r + 1, :] = vec_row(points, a, b)
    for b in range(ng):
        dyn[0][own, 3 * na + b : 3 * na + b + 1, :] = flat_row(base, b)

    for a in range(3):
        for b in range(na):
            tgt_a[b, a] = jnp.transpose(jnp.broadcast_to(vec_row(sites, a, b), (BLOCK, BLOCK)))
        for b in range(ng):
            tgt_g[b, a] = jnp.transpose(jnp.broadcast_to(vec_row(points, a, b), (BLOCK, BLOCK)))

    def inverse_of(dx, dy, dz):
        return lax.rsqrt(dx * dx + dy * dy + dz * dz + soften_sq)

    def store_dipole_pair(slot, targets, source, self_mask):
        dx, dy, dz = (t - s for t, s in zip(targets, source))
        inv = inverse_of(dx, dy, dz)
        cube = inv * inv * inv
        weight = cube * lax.rsqrt(inv) * math.sqrt(3.0)
        geo[slot] = dx * weight
        geo[slot + 1] = dy * weight
        geo[slot + 2] = dz * weight
        geo[slot + 3] = cube if self_mask is None else jnp.where(self_mask, 0.0, cube)

    def store_charge_pair(ref, slot, targets, source):
        dx, dy, dz = (t - s for t, s in zip(targets, source))
        inv = inverse_of(dx, dy, dz)
        cube = inv * inv * inv
        ref[slot] = dx * cube
        ref[slot + 1] = dy * cube
        ref[slot + 2] = dz * cube

    def wide(row):
        return jnp.broadcast_to(row, (SUB, BLOCK))

    def targets_of(ref, b, group):
        return [ref[b, a, pl.ds(group * SUB, SUB), :] for a in range(3)]

    for b in range(na):
        source = [wide(vec_row(sites, a, b)) for a in range(3)]
        for t in range(GROUPS):
            slot = (b * GROUPS + t) * nk * 4
            store_dipole_pair(slot, targets_of(tgt_a, b, t), source, diag == t * SUB)

    greeted = grps - 1
    greeted += has_prev.astype(jnp.int32) * (grps - 1) + has_next.astype(jnp.int32) * (grps - 1)
    greeted += cells - 1
    pl.semaphore_wait(barrier, greeted)

    def piece_copy(buf, send, recv, slot, c, g):
        return pltpu.make_async_remote_copy(
            src_ref=buf.at[own],
            dst_ref=buf.at[slot * grps + grp],
            send_sem=send.at[slot * grps + g],
            recv_sem=recv.at[slot * grps + grp],
            device_id=(c, g),
            device_id_type=MESH,
        )

    def for_peers(buf, send, recv, act):
        for d in range(1, grps):
            g = lax.rem(grp + d, grps)
            act(piece_copy(buf, send, recv, 1, cell, g))

    def for_neighbours(buf, send, recv, act):
        @pl.when(has_prev)
        def _():
            for d in range(grps):
                g = lax.rem(grp + d, grps)
                act(piece_copy(buf, send, recv, 2, cell - 1, g))

        @pl.when(has_next)
        def _():
            for d in range(grps):
                g = lax.rem(grp + d, grps)
                act(piece_copy(buf, send, recv, 0, cell + 1, g))

    def arrival(buf, send, recv, p, c, g):
        pltpu.make_async_remote_copy(
            src_ref=buf.at[p],
            dst_ref=buf.at[p],
            send_sem=send.at[p],
            recv_sem=recv.at[p],
            device_id=(c, g),
            device_id_type=MESH,
        ).wait_recv()

    def peers_arrive(buf, send, recv):
        for d in range(1, grps):
            g = lax.rem(grp + d, grps)
            arrival(buf, send, recv, grps + g, cell, g)

    def neighbours_arrive(buf, send, recv):
        @pl.when(has_prev)
        def _():
            for g in range(grps):
                arrival(buf, send, recv, g, cell - 1, g)

        @pl.when(has_next)
        def _():
            for g in range(grps):
                arrival(buf, send, recv, 2 * grps + g, cell + 1, g)

    def start(copy):
        copy.start()

    def far_copy(it, c):
        return pltpu.make_async_remote_copy(
            src_ref=tab[it].at[cell],
            dst_ref=tab[it].at[cell],
            send_sem=far_send.at[it, c],
            recv_sem=far_recv.at[it, cell],
            device_id=(c, grp),
            device_id_type=MESH,
        )

    def far_arrival(it, c):
        pltpu.make_async_remote_copy(
            src_ref=tab[it].at[c],
            dst_ref=tab[it].at[c],
            send_sem=far_send.at[it, c],
            recv_sem=far_recv.at[it, c],
            device_id=(c, grp),
            device_id_type=MESH,
        ).wait_recv()

    def cell_sums(it):
        rows = []
        total = dyn[it][grps]
        for p in range(1, grps):
            total = total + dyn[it][grps + p]
        for a in range(3):
            rows.append(jnp.sum(total[a * na : (a + 1) * na], axis=0, keepdims=True))
        rows.append(jnp.sum(total[3 * na : 3 * na + ng], axis=0, keepdims=True))
        for a in range(3):
            moment = None
            for p in range(grps):
                q = dyn[it][grps + p, 3 * na : 3 * na + ng, :]
                r = 3 * na + a * ng
                term = q * (stat[grps + p, r : r + ng, :] - centre[a])
                moment = term if moment is None else moment + term
            rows.append(jnp.sum(moment, axis=0, keepdims=True))
        tile = jnp.zeros((SUB, BLOCK), jnp.float32)
        for n, row in enumerate(rows):
            tile = jnp.where(subs == n, wide(row), tile)
        sums = jnp.sum(tile, axis=1, keepdims=True)
        tab[it][cell] = jnp.broadcast_to(sums, (SUB, BLOCK))

    def mm_place(w):
        return lax.div(w, na), lax.rem(w, na)

    def grid_place(w):
        return lax.div(w, ng), lax.rem(w, ng)

    def site_rows(w):
        p, lb = mm_place(w)
        return [wide(stat[p, pl.ds(a * na + lb, 1), :]) for a in range(3)]

    def point_rows(w):
        p, lb = grid_place(w)
        return [wide(stat[p, pl.ds(3 * na + a * ng + lb, 1), :]) for a in range(3)]

    def geometry_atoms(i, carry):
        b = lax.div(i, HALVES)
        first = lax.rem(i, HALVES) * UNROLL
        for k in range(nb):
            source = site_rows(near_s[b, k])
            for t in range(UNROLL):
                slot = ((i * UNROLL + t) * nk + k + 1) * 4
                store_dipole_pair(slot, targets_of(tgt_a, b, first + t), source, None)
        for k in range(nq):
            source = point_rows(grid_s[b, k])
            for t in range(UNROLL):
                slot = ((i * UNROLL + t) * nq + k) * 3
                store_charge_pair(cgeo, slot, targets_of(tgt_a, b, first + t), source)
        return carry

    def geometry_grid(i, carry):
        b = lax.div(i, HALVES)
        first = lax.rem(i, HALVES) * UNROLL
        for k in range(nm):
            source = site_rows(source_s[b, k])
            for t in range(UNROLL):
                slot = ((i * UNROLL + t) * nm + k) * 3
                store_charge_pair(pgeo, slot, targets_of(tgt_g, b, first + t), source)
        return carry

    def near_atoms(it, i, carry):
        b = lax.div(i, HALVES)
        first = lax.rem(i, HALVES) * UNROLL
        acc = [[None] * 3 for _ in range(UNROLL)]
        for k in range(nk):
            p, lb = (own, b) if k == 0 else mm_place(near_s[b, k - 1])
            mu = [wide(dyn[it][p, pl.ds(a * na + lb, 1), :]) for a in range(3)]
            for t in range(UNROLL):
                slot = ((i * UNROLL + t) * nk + k) * 4
                u = [geo[slot + a] for a in range(3)]
                cube = geo[slot + 3]
                proj = u[0] * mu[0] + u[1] * mu[1] + u[2] * mu[2]
                for a in range(3):
                    term = u[a] * proj - cube * mu[a]
                    acc[t][a] = term if k == 0 else acc[t][a] + term
        for k in range(nq):
            p, lb = grid_place(grid_s[b, k])
            q = wide(dyn[it][p, pl.ds(3 * na + lb, 1), :])
            for t in range(UNROLL):
                slot = ((i * UNROLL + t) * nq + k) * 3
                for a in range(3):
                    acc[t][a] = acc[t][a] + cgeo[slot + a] * q
        out = []
        for a in range(3):
            row = jnp.zeros((SUB, BLOCK), jnp.float32)
            for t in range(UNROLL):
                total = jnp.sum(acc[t][a], axis=1, keepdims=True)
                row = jnp.where(diag == (first + t) * SUB, total, row)
            out.append(row)
        for a in range(3):
            fld[i * 3 + a] = out[a]
        return carry

    def near_grid(it, i, carry):
        b = lax.div(i, HALVES)
        first = lax.rem(i, HALVES) * UNROLL
        acc = [None] * UNROLL
        for k in range(nm):
            p, lb = mm_place(source_s[b, k])
            mu = [wide(dyn[it][p, pl.ds(a * na + lb, 1), :]) for a in range(3)]
            for t in range(UNROLL):
                slot = ((i * UNROLL + t) * nm + k) * 3
                term = pgeo[slot] * mu[0] + pgeo[slot + 1] * mu[1] + pgeo[slot + 2] * mu[2]
                acc[t] = term if k == 0 else acc[t] + term
        row = jnp.zeros((SUB, BLOCK), jnp.float32)
        for t in range(UNROLL):
            total = jnp.sum(acc[t], axis=1, keepdims=True)
            row = jnp.where(diag == (first + t) * SUB, total, row)
        fld[na * HALVES * 3 + i] = row
        return carry

    def far_geometry(row_of):
        c = lax.broadcasted_iota(jnp.int32, (cells, BLOCK), 0)
        dx = row_of(0) - (c.astype(jnp.float32) + 0.5)
        dy = jnp.broadcast_to(row_of(1) - 0.5, (cells, BLOCK))
        dz = jnp.broadcast_to(row_of(2) - 0.5, (cells, BLOCK))
        inv = inverse_of(dx, dy, dz)
        cube = jnp.where(jnp.abs(c - cell) >= 2, inv * inv * inv, 0.0)
        return (dx, dy, dz), cube, cube * inv * inv * 3.0

    def column_sum(x):
        return jnp.sum(x, axis=0, keepdims=True)

    for_peers(stat, stat_send, stat_recv, start)
    for_peers(dyn[0], dyn_send.at[0], dyn_recv.at[0], start)
    for_neighbours(stat, stat_send, stat_recv, start)
    for_neighbours(dyn[0], dyn_send.at[0], dyn_recv.at[0], start)
    peers_arrive(stat, stat_send, stat_recv)

    for it in range(ITERS):
        send, recv = dyn_send.at[it], dyn_recv.at[it]
        if it > 0:
            for_peers(dyn[it], send, recv, start)
            for_neighbours(dyn[it], send, recv, start)
        peers_arrive(dyn[it], send, recv)
        cell_sums(it)
        each_far(lambda c: far_copy(it, c).start())
        if it == 0:
            neighbours_arrive(stat, stat_send, stat_recv)
            lax.fori_loop(0, na * HALVES, geometry_atoms, 0)
            lax.fori_loop(0, ng * HALVES, geometry_grid, 0)
        neighbours_arrive(dyn[it], send, recv)
        lax.fori_loop(0, na * HALVES, functools.partial(near_atoms, it), 0)
        lax.fori_loop(0, ng * HALVES, functools.partial(near_grid, it), 0)
        each_far(lambda c: far_arrival(it, c))
        sums = [tab[it][:, n, :] for n in range(7)]
        moments = [sums[a] + sums[4 + a] for a in range(3)]
        for b in range(na):
            delta, cube, fifth = far_geometry(lambda a: vec_row(sites, a, b))
            radial = fifth * (moments[0] * delta[0] + moments[1] * delta[1] + moments[2] * delta[2])
            radial = radial + sums[3] * cube
            for a in range(3):
                far = column_sum(radial * delta[a] - moments[a] * cube)
                near = fld[b * HALVES * 3 + a]
                for h in range(1, HALVES):
                    near = near + fld[(b * HALVES + h) * 3 + a]
                new = flat_row(pol, b) * (vec_row(fixed, a, b) + (column_sum(near) + far))
                if it + 1 < ITERS:
                    dyn[it + 1][own, a * na + b : a * na + b + 1, :] = new
                else:
                    out_dip[a : a + 1, b * BLOCK : (b + 1) * BLOCK] = new
        for b in range(ng):
            delta, cube, _ = far_geometry(lambda a: vec_row(points, a, b))
            proj = sums[0] * delta[0] + sums[1] * delta[1] + sums[2] * delta[2]
            far = column_sum(proj * cube)
            slot = na * HALVES * 3 + b * HALVES
            near = fld[slot]
            for h in range(1, HALVES):
                near = near + fld[slot + h]
            new = flat_row(base, b) - flat_row(resp, b) * (column_sum(near) + far)
            if it + 1 < ITERS:
                dyn[it + 1][own, 3 * na + b : 3 * na + b + 1, :] = new
            else:
                out_q[b * BLOCK : (b + 1) * BLOCK] = new.reshape(BLOCK)

    def finish(copy):
        copy.wait_send()

    for_peers(stat, stat_send, stat_recv, finish)
    for_neighbours(stat, stat_send, stat_recv, finish)
    for it in range(ITERS):
        for_peers(dyn[it], dyn_send.at[it], dyn_recv.at[it], finish)
        for_neighbours(dyn[it], dyn_send.at[it], dyn_recv.at[it], finish)
        each_far(lambda c: far_copy(it, c).wait_send())


def solution(mesh):
    cells, grps = mesh.shape["cell"], mesh.shape["grp"]

    def step(sites, points, guess, fixed, pol, base, resp, near, grid, source):
        na, nb = near.shape
        nq = grid.shape[1]
        ng, nm = source.shape
        stat_rows = round_up(3 * na + 3 * ng, SUB)
        dyn_rows = round_up(3 * na + ng, SUB)
        f32 = jnp.float32
        smem = pl.BlockSpec(memory_space=pltpu.SMEM)
        vmem = pl.BlockSpec(memory_space=pltpu.VMEM)
        dma = pltpu.SemaphoreType.DMA
        return pl.pallas_call(
            functools.partial(body, (cells, grps, na, ng, nb, nq, nm)),
            out_shape=(
                jax.ShapeDtypeStruct(sites.shape, f32),
                jax.ShapeDtypeStruct(base.shape, f32),
            ),
            in_specs=[smem] * 3 + [vmem] * 7,
            out_specs=(vmem, vmem),
            scratch_shapes=[pltpu.VMEM((3 * grps, stat_rows, BLOCK), f32)]
            + [pltpu.VMEM((3 * grps, dyn_rows, BLOCK), f32) for _ in range(ITERS)]
            + [pltpu.VMEM((cells, SUB, BLOCK), f32) for _ in range(ITERS)]
            + [
                pltpu.VMEM((na, 3, BLOCK, BLOCK), f32),
                pltpu.VMEM((ng, 3, BLOCK, BLOCK), f32),
                pltpu.VMEM((na * GROUPS * (nb + 1) * 4, SUB, BLOCK), f32),
                pltpu.VMEM((na * GROUPS * nq * 3, SUB, BLOCK), f32),
                pltpu.VMEM((ng * GROUPS * nm * 3, SUB, BLOCK), f32),
                pltpu.VMEM(((na * 3 + ng) * HALVES, SUB, BLOCK), f32),
                dma((3 * grps,)),
                dma((3 * grps,)),
                dma((ITERS, 3 * grps)),
                dma((ITERS, 3 * grps)),
                dma((ITERS, cells)),
                dma((ITERS, cells)),
            ],
            compiler_params=pltpu.CompilerParams(collective_id=0, has_side_effects=True),
        )(near, grid, source, sites, points, guess, fixed, pol, base, resp)

    pair = P(("cell", "grp"))
    wide = P(None, ("cell", "grp"))
    tall = P(("cell", "grp"), None)
    return jax.shard_map(
        step,
        mesh=mesh,
        in_specs=(wide, wide, wide, wide, pair, pair, pair, tall, tall, tall),
        out_specs=(wide, pair),
        check_vma=False,
    )
```

```python
import functools
import math

import jax
import jax.numpy as jnp
from jax import lax
from jax.experimental import pallas as pl
from jax.experimental.pallas import tpu as pltpu
from jax.sharding import PartitionSpec as P

BLOCK = 128
SUB = 8
GROUPS = BLOCK // SUB
UNROLL = 8
HALVES = GROUPS // UNROLL
ITERS = 3
MESH = pl.DeviceIdType.MESH

soften_sq = 0.04


def round_up(n, m):
    return (n + m - 1) // m * m


def body(dims, *refs):
    cells, grps, na, ng, nb, nq, nm = dims
    args, (out_dip, out_q), held = refs[:10], refs[10:12], refs[12:22]
    near_s, grid_s, source_s, sites, points, guess, fixed, pol, base, resp = held
    stat = refs[22]
    dyn = refs[23 : 23 + ITERS]
    tab = refs[23 + ITERS : 23 + 2 * ITERS]
    rest = refs[23 + 2 * ITERS :]
    tgt_a, tgt_g, geo, cgeo, pgeo, fld = rest[:6]
    load_sem, stat_send, stat_recv, dyn_send, dyn_recv, far_send, far_recv = rest[6:]
    cell = lax.axis_index("cell")
    grp = lax.axis_index("grp")
    has_prev = cell > 0
    has_next = cell < cells - 1
    nk = nb + 1
    own = grps + grp
    cell_f = cell.astype(jnp.float32)
    centre = (cell_f + 0.5, 0.5, 0.5)

    def vec_row(ref, a, b):
        return ref[a : a + 1, b * BLOCK : (b + 1) * BLOCK]

    def flat_row(ref, b):
        return ref[b * BLOCK : (b + 1) * BLOCK].reshape(1, BLOCK)

    lanes = lax.broadcasted_iota(jnp.int32, (SUB, BLOCK), 1)
    subs = lax.broadcasted_iota(jnp.int32, (SUB, BLOCK), 0)
    diag = lanes - subs

    for it in range(ITERS):
        tab[it][...] = jnp.zeros_like(tab[it])

    @pl.when(jnp.logical_not(has_prev))
    def _():
        for p in range(grps):
            stat[p] = jnp.zeros(stat.shape[1:], jnp.float32)
            for it in range(ITERS):
                dyn[it][p] = jnp.zeros(dyn[it].shape[1:], jnp.float32)

    @pl.when(jnp.logical_not(has_next))
    def _():
        for p in range(2 * grps, 3 * grps):
            stat[p] = jnp.zeros(stat.shape[1:], jnp.float32)
            for it in range(ITERS):
                dyn[it][p] = jnp.zeros(dyn[it].shape[1:], jnp.float32)

    barrier = pltpu.get_barrier_semaphore()

    def greet(c, g):
        pl.semaphore_signal(barrier, inc=1, device_id=(c, g), device_id_type=MESH)

    def each_other_cell(act):
        def step(n, carry):
            c = lax.rem(cell + n, cells)
            for d in range(grps):
                act(c, lax.rem(grp + d, grps))
            return carry

        lax.fori_loop(1, cells, step, 0)

    each_other_cell(greet)
    for d in range(1, grps):
        greet(cell, lax.rem(grp + d, grps))

    loads = [
        pltpu.make_async_copy(src, dst, load_sem.at[n])
        for n, (src, dst) in enumerate(zip(args, held))
    ]
    for load in loads:
        load.start()
    for load in loads:
        load.wait()

    for a in range(3):
        for b in range(na):
            stat[own, a * na + b : a * na + b + 1, :] = vec_row(sites, a, b)
            dyn[0][own, a * na + b : a * na + b + 1, :] = vec_row(guess, a, b)
        for b in range(ng):
            r = 3 * na + a * ng + b
            stat[own, r : r + 1, :] = vec_row(points, a, b)
    for b in range(ng):
        dyn[0][own, 3 * na + b : 3 * na + b + 1, :] = flat_row(base, b)

    for a in range(3):
        for b in range(na):
            tgt_a[b, a] = jnp.transpose(jnp.broadcast_to(vec_row(sites, a, b), (BLOCK, BLOCK)))
        for b in range(ng):
            tgt_g[b, a] = jnp.transpose(jnp.broadcast_to(vec_row(points, a, b), (BLOCK, BLOCK)))

    def inverse_of(dx, dy, dz):
        return lax.rsqrt(dx * dx + dy * dy + dz * dz + soften_sq)

    def store_dipole_pair(slot, targets, source, self_mask):
        dx, dy, dz = (t - s for t, s in zip(targets, source))
        inv = inverse_of(dx, dy, dz)
        cube = inv * inv * inv
        weight = cube * lax.rsqrt(inv) * math.sqrt(3.0)
        geo[slot] = dx * weight
        geo[slot + 1] = dy * weight
        geo[slot + 2] = dz * weight
        geo[slot + 3] = cube if self_mask is None else jnp.where(self_mask, 0.0, cube)

    def store_charge_pair(ref, slot, targets, source):
        dx, dy, dz = (t - s for t, s in zip(targets, source))
        inv = inverse_of(dx, dy, dz)
        cube = inv * inv * inv
        ref[slot] = dx * cube
        ref[slot + 1] = dy * cube
        ref[slot + 2] = dz * cube

    def column_sum(x):
        return jnp.sum(x, axis=0, keepdims=True)

    def wide(row):
        return jnp.broadcast_to(row, (SUB, BLOCK))

    def targets_of(ref, b, group):
        return [ref[b, a, pl.ds(group * SUB, SUB), :] for a in range(3)]

    for b in range(na):
        source = [wide(vec_row(sites, a, b)) for a in range(3)]
        for t in range(GROUPS):
            slot = (b * GROUPS + t) * nk * 4
            store_dipole_pair(slot, targets_of(tgt_a, b, t), source, diag == t * SUB)

    pl.semaphore_wait(barrier, cells * grps - 1)

    def piece_copy(buf, send, recv, slot, c, g):
        return pltpu.make_async_remote_copy(
            src_ref=buf.at[own],
            dst_ref=buf.at[slot * grps + grp],
            send_sem=send.at[slot * grps + g],
            recv_sem=recv.at[slot * grps + grp],
            device_id=(c, g),
            device_id_type=MESH,
        )

    def for_peers(buf, send, recv, act):
        for d in range(1, grps):
            g = lax.rem(grp + d, grps)
            act(piece_copy(buf, send, recv, 1, cell, g))

    def for_neighbours(buf, send, recv, act):
        @pl.when(has_prev)
        def _():
            for d in range(grps):
                g = lax.rem(grp + d, grps)
                act(piece_copy(buf, send, recv, 2, cell - 1, g))

        @pl.when(has_next)
        def _():
            for d in range(grps):
                g = lax.rem(grp + d, grps)
                act(piece_copy(buf, send, recv, 0, cell + 1, g))

    def arrival(buf, send, recv, p, c, g):
        pltpu.make_async_remote_copy(
            src_ref=buf.at[p],
            dst_ref=buf.at[p],
            send_sem=send.at[p],
            recv_sem=recv.at[p],
            device_id=(c, g),
            device_id_type=MESH,
        ).wait_recv()

    def peers_arrive(buf, send, recv):
        for d in range(1, grps):
            g = lax.rem(grp + d, grps)
            arrival(buf, send, recv, grps + g, cell, g)

    def neighbours_arrive(buf, send, recv):
        @pl.when(has_prev)
        def _():
            for g in range(grps):
                arrival(buf, send, recv, g, cell - 1, g)

        @pl.when(has_next)
        def _():
            for g in range(grps):
                arrival(buf, send, recv, 2 * grps + g, cell + 1, g)

    def start(copy):
        copy.start()

    def far_row(it, c, g):
        return tab[it].at[pl.ds(g * cells + c, 1)]

    def far_copy(it, c, g):
        return pltpu.make_async_remote_copy(
            src_ref=far_row(it, cell, grp),
            dst_ref=far_row(it, cell, grp),
            send_sem=far_send.at[it],
            recv_sem=far_recv.at[it],
            device_id=(c, g),
            device_id_type=MESH,
        )

    def far_all(it):
        rows = tab[it].at[pl.ds(0, (cells - 1) * grps)]
        return pltpu.make_async_remote_copy(
            src_ref=rows,
            dst_ref=rows,
            send_sem=far_send.at[it],
            recv_sem=far_recv.at[it],
            device_id=(lax.rem(cell + 1, cells), grp),
            device_id_type=MESH,
        )

    def own_sums(it):
        mine = dyn[it][own]
        rows = [column_sum(mine[a * na : (a + 1) * na]) for a in range(3)]
        q = mine[3 * na : 3 * na + ng]
        rows.append(column_sum(q))
        for a in range(3):
            r = 3 * na + a * ng
            rows.append(column_sum(q * (stat[own, r : r + ng, :] - centre[a])))
        tile = jnp.zeros((SUB, BLOCK), jnp.float32)
        for n, row in enumerate(rows):
            tile = jnp.where(subs == n, wide(row), tile)
        sums = jnp.sum(tile, axis=1, keepdims=True)
        tab[it][grp * cells + cell] = column_sum(jnp.where(diag == 0, sums, 0.0))

    def far_sums(it):
        total = tab[it][0:cells, 0, :]
        for g in range(1, grps):
            total = total + tab[it][g * cells : (g + 1) * cells, 0, :]
        return [jnp.broadcast_to(total[:, n : n + 1], (cells, BLOCK)) for n in range(7)]

    def mm_place(w):
        return lax.div(w, na), lax.rem(w, na)

    def grid_place(w):
        return lax.div(w, ng), lax.rem(w, ng)

    def site_rows(w):
        p, lb = mm_place(w)
        return [wide(stat[p, pl.ds(a * na + lb, 1), :]) for a in range(3)]

    def point_rows(w):
        p, lb = grid_place(w)
        return [wide(stat[p, pl.ds(3 * na + a * ng + lb, 1), :]) for a in range(3)]

    def geometry_atoms(i, carry):
        b = lax.div(i, HALVES)
        first = lax.rem(i, HALVES) * UNROLL
        for k in range(nb):
            source = site_rows(near_s[b, k])
            for t in range(UNROLL):
                slot = ((i * UNROLL + t) * nk + k + 1) * 4
                store_dipole_pair(slot, targets_of(tgt_a, b, first + t), source, None)
        for k in range(nq):
            source = point_rows(grid_s[b, k])
            for t in range(UNROLL):
                slot = ((i * UNROLL + t) * nq + k) * 3
                store_charge_pair(cgeo, slot, targets_of(tgt_a, b, first + t), source)
        return carry

    def geometry_grid(i, carry):
        b = lax.div(i, HALVES)
        first = lax.rem(i, HALVES) * UNROLL
        for k in range(nm):
            source = site_rows(source_s[b, k])
            for t in range(UNROLL):
                slot = ((i * UNROLL + t) * nm + k) * 3
                store_charge_pair(pgeo, slot, targets_of(tgt_g, b, first + t), source)
        return carry

    def near_atoms(it, i, carry):
        b = lax.div(i, HALVES)
        first = lax.rem(i, HALVES) * UNROLL
        acc = [[None] * 3 for _ in range(UNROLL)]
        for k in range(nk):
            p, lb = (own, b) if k == 0 else mm_place(near_s[b, k - 1])
            mu = [wide(dyn[it][p, pl.ds(a * na + lb, 1), :]) for a in range(3)]
            for t in range(UNROLL):
                slot = ((i * UNROLL + t) * nk + k) * 4
                u = [geo[slot + a] for a in range(3)]
                cube = geo[slot + 3]
                proj = u[0] * mu[0] + u[1] * mu[1] + u[2] * mu[2]
                for a in range(3):
                    term = u[a] * proj - cube * mu[a]
                    acc[t][a] = term if k == 0 else acc[t][a] + term
        for k in range(nq):
            p, lb = grid_place(grid_s[b, k])
            q = wide(dyn[it][p, pl.ds(3 * na + lb, 1), :])
            for t in range(UNROLL):
                slot = ((i * UNROLL + t) * nq + k) * 3
                for a in range(3):
                    acc[t][a] = acc[t][a] + cgeo[slot + a] * q
        out = []
        for a in range(3):
            row = jnp.zeros((SUB, BLOCK), jnp.float32)
            for t in range(UNROLL):
                total = jnp.sum(acc[t][a], axis=1, keepdims=True)
                row = jnp.where(diag == (first + t) * SUB, total, row)
            out.append(row)
        for a in range(3):
            fld[i * 3 + a] = out[a]
        return carry

    def near_grid(it, i, carry):
        b = lax.div(i, HALVES)
        first = lax.rem(i, HALVES) * UNROLL
        acc = [None] * UNROLL
        for k in range(nm):
            p, lb = mm_place(source_s[b, k])
            mu = [wide(dyn[it][p, pl.ds(a * na + lb, 1), :]) for a in range(3)]
            for t in range(UNROLL):
                slot = ((i * UNROLL + t) * nm + k) * 3
                term = pgeo[slot] * mu[0] + pgeo[slot + 1] * mu[1] + pgeo[slot + 2] * mu[2]
                acc[t] = term if k == 0 else acc[t] + term
        row = jnp.zeros((SUB, BLOCK), jnp.float32)
        for t in range(UNROLL):
            total = jnp.sum(acc[t], axis=1, keepdims=True)
            row = jnp.where(diag == (first + t) * SUB, total, row)
        fld[na * HALVES * 3 + i] = row
        return carry

    def far_geometry(row_of):
        c = lax.broadcasted_iota(jnp.int32, (cells, BLOCK), 0)
        dx = row_of(0) - (c.astype(jnp.float32) + 0.5)
        dy = jnp.broadcast_to(row_of(1) - 0.5, (cells, BLOCK))
        dz = jnp.broadcast_to(row_of(2) - 0.5, (cells, BLOCK))
        inv = inverse_of(dx, dy, dz)
        cube = jnp.where(jnp.abs(c - cell) >= 2, inv * inv * inv, 0.0)
        return (dx, dy, dz), cube, cube * inv * inv * 3.0

    for_peers(stat, stat_send, stat_recv, start)
    for_peers(dyn[0], dyn_send.at[0], dyn_recv.at[0], start)
    for_neighbours(stat, stat_send, stat_recv, start)
    for_neighbours(dyn[0], dyn_send.at[0], dyn_recv.at[0], start)

    for it in range(ITERS):
        send, recv = dyn_send.at[it], dyn_recv.at[it]
        if it > 0:
            for_peers(dyn[it], send, recv, start)
            for_neighbours(dyn[it], send, recv, start)
        own_sums(it)
        each_other_cell(lambda c, g: far_copy(it, c, g).start())
        if it == 0:
            peers_arrive(stat, stat_send, stat_recv)
            neighbours_arrive(stat, stat_send, stat_recv)
            lax.fori_loop(0, na * HALVES, geometry_atoms, 0)
            lax.fori_loop(0, ng * HALVES, geometry_grid, 0)
        peers_arrive(dyn[it], send, recv)
        neighbours_arrive(dyn[it], send, recv)
        lax.fori_loop(0, na * HALVES, functools.partial(near_atoms, it), 0)
        lax.fori_loop(0, ng * HALVES, functools.partial(near_grid, it), 0)
        far_all(it).wait_recv()
        sums = far_sums(it)
        moments = [sums[a] + sums[4 + a] for a in range(3)]
        for b in range(na):
            delta, cube, fifth = far_geometry(lambda a: vec_row(sites, a, b))
            radial = fifth * (moments[0] * delta[0] + moments[1] * delta[1] + moments[2] * delta[2])
            radial = radial + sums[3] * cube
            for a in range(3):
                far = column_sum(radial * delta[a] - moments[a] * cube)
                near = fld[b * HALVES * 3 + a]
                for h in range(1, HALVES):
                    near = near + fld[(b * HALVES + h) * 3 + a]
                new = flat_row(pol, b) * (vec_row(fixed, a, b) + (column_sum(near) + far))
                if it + 1 < ITERS:
                    dyn[it + 1][own, a * na + b : a * na + b + 1, :] = new
                else:
                    out_dip[a : a + 1, b * BLOCK : (b + 1) * BLOCK] = new
        for b in range(ng):
            delta, cube, _ = far_geometry(lambda a: vec_row(points, a, b))
            proj = sums[0] * delta[0] + sums[1] * delta[1] + sums[2] * delta[2]
            far = column_sum(proj * cube)
            slot = na * HALVES * 3 + b * HALVES
            near = fld[slot]
            for h in range(1, HALVES):
                near = near + fld[slot + h]
            new = flat_row(base, b) - flat_row(resp, b) * (column_sum(near) + far)
            if it + 1 < ITERS:
                dyn[it + 1][own, 3 * na + b : 3 * na + b + 1, :] = new
            else:
                out_q[b * BLOCK : (b + 1) * BLOCK] = new.reshape(BLOCK)

    def finish(copy):
        copy.wait_send()

    for_peers(stat, stat_send, stat_recv, finish)
    for_neighbours(stat, stat_send, stat_recv, finish)
    for it in range(ITERS):
        for_peers(dyn[it], dyn_send.at[it], dyn_recv.at[it], finish)
        for_neighbours(dyn[it], dyn_send.at[it], dyn_recv.at[it], finish)
        far_all(it).wait_send()


def solution(mesh):
    cells, grps = mesh.shape["cell"], mesh.shape["grp"]

    def step(sites, points, guess, fixed, pol, base, resp, near, grid, source):
        na, nb = near.shape
        nq = grid.shape[1]
        ng, nm = source.shape
        stat_rows = round_up(3 * na + 3 * ng, SUB)
        dyn_rows = round_up(3 * na + ng, SUB)
        f32 = jnp.float32
        args = (near, grid, source, sites, points, guess, fixed, pol, base, resp)
        vmem = pl.BlockSpec(memory_space=pltpu.VMEM)
        dma = pltpu.SemaphoreType.DMA
        return pl.pallas_call(
            functools.partial(body, (cells, grps, na, ng, nb, nq, nm)),
            out_shape=(
                jax.ShapeDtypeStruct(sites.shape, f32),
                jax.ShapeDtypeStruct(base.shape, f32),
            ),
            in_specs=[pl.BlockSpec(memory_space=pl.ANY)] * 10,
            out_specs=(vmem, vmem),
            scratch_shapes=[pltpu.SMEM(x.shape, x.dtype) for x in args[:3]]
            + [pltpu.VMEM(x.shape, x.dtype) for x in args[3:]]
            + [pltpu.VMEM((3 * grps, stat_rows, BLOCK), f32)]
            + [pltpu.VMEM((3 * grps, dyn_rows, BLOCK), f32) for _ in range(ITERS)]
            + [pltpu.VMEM((cells * grps, 1, BLOCK), f32) for _ in range(ITERS)]
            + [
                pltpu.VMEM((na, 3, BLOCK, BLOCK), f32),
                pltpu.VMEM((ng, 3, BLOCK, BLOCK), f32),
                pltpu.VMEM((na * GROUPS * (nb + 1) * 4, SUB, BLOCK), f32),
                pltpu.VMEM((na * GROUPS * nq * 3, SUB, BLOCK), f32),
                pltpu.VMEM((ng * GROUPS * nm * 3, SUB, BLOCK), f32),
                pltpu.VMEM(((na * 3 + ng) * HALVES, SUB, BLOCK), f32),
                dma((10,)),
                dma((3 * grps,)),
                dma((3 * grps,)),
                dma((ITERS, 3 * grps)),
                dma((ITERS, 3 * grps)),
                dma((ITERS,)),
                dma((ITERS,)),
            ],
            compiler_params=pltpu.CompilerParams(collective_id=0, has_side_effects=True),
        )(*args)

    pair = P(("cell", "grp"))
    wide = P(None, ("cell", "grp"))
    tall = P(("cell", "grp"), None)
    return jax.shard_map(
        step,
        mesh=mesh,
        in_specs=(wide, wide, wide, wide, pair, pair, pair, tall, tall, tall),
        out_specs=(wide, pair),
        check_vma=False,
    )
```

```python
import functools
import math

import jax
import jax.numpy as jnp
from jax import lax
from jax.experimental import pallas as pl
from jax.experimental.pallas import tpu as pltpu
from jax.sharding import PartitionSpec as P

BLOCK = 128
SUB = 8
GROUPS = BLOCK // SUB
UNROLL = 8
HALVES = GROUPS // UNROLL
ITERS = 3
MESH = pl.DeviceIdType.MESH

soften_sq = 0.04


def round_up(n, m):
    return (n + m - 1) // m * m


def body(dims, *refs):
    cells, grps, na, ng, nb, nq, nm = dims
    args, (out_dip, out_q), held = refs[:10], refs[10:12], refs[12:22]
    near_s, grid_s, source_s, sites, points, guess, fixed, pol, base, resp = held
    stat = refs[22]
    dyn = refs[23 : 23 + ITERS]
    tab = refs[23 + ITERS : 23 + 2 * ITERS]
    rest = refs[23 + 2 * ITERS :]
    tgt_a, tgt_g, geo, cgeo, pgeo, fld, selfs = rest[:7]
    load_sem, stat_send, stat_recv, dyn_send, dyn_recv, far_send, far_recv = rest[7:]
    cell = lax.axis_index("cell")
    grp = lax.axis_index("grp")
    has_prev = cell > 0
    has_next = cell < cells - 1
    nk = nb + 1
    own = grps + grp
    cell_f = cell.astype(jnp.float32)
    centre = (cell_f + 0.5, 0.5, 0.5)

    def vec_row(ref, a, b):
        return ref[a : a + 1, b * BLOCK : (b + 1) * BLOCK]

    def flat_row(ref, b):
        return ref[b * BLOCK : (b + 1) * BLOCK].reshape(1, BLOCK)

    lanes = lax.broadcasted_iota(jnp.int32, (SUB, BLOCK), 1)
    subs = lax.broadcasted_iota(jnp.int32, (SUB, BLOCK), 0)
    diag = lanes - subs

    for it in range(ITERS):
        tab[it][...] = jnp.zeros_like(tab[it])

    @pl.when(jnp.logical_not(has_prev))
    def _():
        for p in range(grps):
            stat[p] = jnp.zeros(stat.shape[1:], jnp.float32)
            for it in range(ITERS):
                dyn[it][p] = jnp.zeros(dyn[it].shape[1:], jnp.float32)

    @pl.when(jnp.logical_not(has_next))
    def _():
        for p in range(2 * grps, 3 * grps):
            stat[p] = jnp.zeros(stat.shape[1:], jnp.float32)
            for it in range(ITERS):
                dyn[it][p] = jnp.zeros(dyn[it].shape[1:], jnp.float32)

    barrier = pltpu.get_barrier_semaphore()

    def greet(c, g):
        pl.semaphore_signal(barrier, inc=1, device_id=(c, g), device_id_type=MESH)

    def each_other_cell(act):
        def step(n, carry):
            c = lax.rem(cell + n, cells)
            for d in range(grps):
                act(c, lax.rem(grp + d, grps))
            return carry

        lax.fori_loop(1, cells, step, 0)

    each_other_cell(greet)
    for d in range(1, grps):
        greet(cell, lax.rem(grp + d, grps))

    loads = [
        pltpu.make_async_copy(src, dst, load_sem.at[n])
        for n, (src, dst) in enumerate(zip(args, held))
    ]
    for load in loads:
        load.start()
    for load in loads:
        load.wait()

    for a in range(3):
        for b in range(na):
            stat[own, a * na + b : a * na + b + 1, :] = vec_row(sites, a, b)
            dyn[0][own, a * na + b : a * na + b + 1, :] = vec_row(guess, a, b)
        for b in range(ng):
            r = 3 * na + a * ng + b
            stat[own, r : r + 1, :] = vec_row(points, a, b)
    for b in range(ng):
        dyn[0][own, 3 * na + b : 3 * na + b + 1, :] = flat_row(base, b)

    for a in range(3):
        for b in range(na):
            tgt_a[b, a] = jnp.transpose(jnp.broadcast_to(vec_row(sites, a, b), (BLOCK, BLOCK)))
        for b in range(ng):
            tgt_g[b, a] = jnp.transpose(jnp.broadcast_to(vec_row(points, a, b), (BLOCK, BLOCK)))

    def inverse_of(dx, dy, dz):
        return lax.rsqrt(dx * dx + dy * dy + dz * dz + soften_sq)

    def store_dipole_pair(slot, targets, source, self_mask):
        dx, dy, dz = (t - s for t, s in zip(targets, source))
        inv = inverse_of(dx, dy, dz)
        cube = inv * inv * inv
        weight = cube * lax.rsqrt(inv) * math.sqrt(3.0)
        geo[slot] = dx * weight
        geo[slot + 1] = dy * weight
        geo[slot + 2] = dz * weight
        geo[slot + 3] = cube if self_mask is None else jnp.where(self_mask, 0.0, cube)

    def store_charge_pair(ref, slot, targets, source):
        dx, dy, dz = (t - s for t, s in zip(targets, source))
        inv = inverse_of(dx, dy, dz)
        cube = inv * inv * inv
        ref[slot] = dx * cube
        ref[slot + 1] = dy * cube
        ref[slot + 2] = dz * cube

    def column_sum(x):
        return jnp.sum(x, axis=0, keepdims=True)

    def wide(row):
        return jnp.broadcast_to(row, (SUB, BLOCK))

    def targets_of(ref, b, group):
        return [ref[b, a, pl.ds(group * SUB, SUB), :] for a in range(3)]

    for b in range(na):
        source = [wide(vec_row(sites, a, b)) for a in range(3)]
        for t in range(GROUPS):
            slot = (b * GROUPS + t) * nk * 4
            store_dipole_pair(slot, targets_of(tgt_a, b, t), source, diag == t * SUB)

    pl.semaphore_wait(barrier, cells * grps - 1)

    def piece_copy(buf, send, recv, slot, c, g):
        return pltpu.make_async_remote_copy(
            src_ref=buf.at[own],
            dst_ref=buf.at[slot * grps + grp],
            send_sem=send.at[slot * grps + g],
            recv_sem=recv.at[slot * grps + grp],
            device_id=(c, g),
            device_id_type=MESH,
        )

    def for_peers(buf, send, recv, act):
        for d in range(1, grps):
            g = lax.rem(grp + d, grps)
            act(piece_copy(buf, send, recv, 1, cell, g))

    def for_neighbours(buf, send, recv, act):
        @pl.when(has_prev)
        def _():
            for d in range(grps):
                g = lax.rem(grp + d, grps)
                act(piece_copy(buf, send, recv, 2, cell - 1, g))

        @pl.when(has_next)
        def _():
            for d in range(grps):
                g = lax.rem(grp + d, grps)
                act(piece_copy(buf, send, recv, 0, cell + 1, g))

    def arrival(buf, send, recv, p, c, g):
        pltpu.make_async_remote_copy(
            src_ref=buf.at[p],
            dst_ref=buf.at[p],
            send_sem=send.at[p],
            recv_sem=recv.at[p],
            device_id=(c, g),
            device_id_type=MESH,
        ).wait_recv()

    def peers_arrive(buf, send, recv):
        for d in range(1, grps):
            g = lax.rem(grp + d, grps)
            arrival(buf, send, recv, grps + g, cell, g)

    def neighbours_arrive(buf, send, recv):
        @pl.when(has_prev)
        def _():
            for g in range(grps):
                arrival(buf, send, recv, g, cell - 1, g)

        @pl.when(has_next)
        def _():
            for g in range(grps):
                arrival(buf, send, recv, 2 * grps + g, cell + 1, g)

    def start(copy):
        copy.start()

    def far_row(it, c, g):
        return tab[it].at[pl.ds(g * cells + c, 1)]

    def far_copy(it, c, g):
        return pltpu.make_async_remote_copy(
            src_ref=far_row(it, cell, grp),
            dst_ref=far_row(it, cell, grp),
            send_sem=far_send.at[it],
            recv_sem=far_recv.at[it],
            device_id=(c, g),
            device_id_type=MESH,
        )

    def far_all(it):
        rows = tab[it].at[pl.ds(0, (cells - 1) * grps)]
        return pltpu.make_async_remote_copy(
            src_ref=rows,
            dst_ref=rows,
            send_sem=far_send.at[it],
            recv_sem=far_recv.at[it],
            device_id=(lax.rem(cell + 1, cells), grp),
            device_id_type=MESH,
        )

    def own_sums(it):
        mine = dyn[it][own]
        rows = [column_sum(mine[a * na : (a + 1) * na]) for a in range(3)]
        q = mine[3 * na : 3 * na + ng]
        rows.append(column_sum(q))
        for a in range(3):
            r = 3 * na + a * ng
            rows.append(column_sum(q * (stat[own, r : r + ng, :] - centre[a])))
        tile = jnp.zeros((SUB, BLOCK), jnp.float32)
        for n, row in enumerate(rows):
            tile = jnp.where(subs == n, wide(row), tile)
        sums = jnp.sum(tile, axis=1, keepdims=True)
        tab[it][grp * cells + cell] = column_sum(jnp.where(diag == 0, sums, 0.0))

    def far_sums(it):
        total = tab[it][0:cells, 0, :]
        for g in range(1, grps):
            total = total + tab[it][g * cells : (g + 1) * cells, 0, :]
        return [jnp.broadcast_to(total[:, n : n + 1], (cells, BLOCK)) for n in range(7)]

    def mm_place(w):
        return lax.div(w, na), lax.rem(w, na)

    def grid_place(w):
        return lax.div(w, ng), lax.rem(w, ng)

    def site_rows(w):
        p, lb = mm_place(w)
        return [wide(stat[p, pl.ds(a * na + lb, 1), :]) for a in range(3)]

    def point_rows(w):
        p, lb = grid_place(w)
        return [wide(stat[p, pl.ds(3 * na + a * ng + lb, 1), :]) for a in range(3)]

    def geometry_atoms(i, carry):
        b = lax.div(i, HALVES)
        first = lax.rem(i, HALVES) * UNROLL
        for k in range(nb):
            source = site_rows(near_s[b, k])
            for t in range(UNROLL):
                slot = ((i * UNROLL + t) * nk + k + 1) * 4
                store_dipole_pair(slot, targets_of(tgt_a, b, first + t), source, None)
        for k in range(nq):
            source = point_rows(grid_s[b, k])
            for t in range(UNROLL):
                slot = ((i * UNROLL + t) * nq + k) * 3
                store_charge_pair(cgeo, slot, targets_of(tgt_a, b, first + t), source)
        return carry

    def geometry_grid(i, carry):
        b = lax.div(i, HALVES)
        first = lax.rem(i, HALVES) * UNROLL
        for k in range(nm):
            source = site_rows(source_s[b, k])
            for t in range(UNROLL):
                slot = ((i * UNROLL + t) * nm + k) * 3
                store_charge_pair(pgeo, slot, targets_of(tgt_g, b, first + t), source)
        return carry

    def self_atoms(it, i, carry):
        b = lax.div(i, HALVES)
        mu = [wide(dyn[it][own, pl.ds(a * na + b, 1), :]) for a in range(3)]
        for t in range(UNROLL):
            slot = (i * UNROLL + t) * nk * 4
            u = [geo[slot + a] for a in range(3)]
            cube = geo[slot + 3]
            proj = u[0] * mu[0] + u[1] * mu[1] + u[2] * mu[2]
            for a in range(3):
                selfs[(i * UNROLL + t) * 3 + a] = u[a] * proj - cube * mu[a]
        return carry

    def near_atoms(it, i, carry):
        b = lax.div(i, HALVES)
        first = lax.rem(i, HALVES) * UNROLL
        acc = [[selfs[(i * UNROLL + t) * 3 + a] for a in range(3)] for t in range(UNROLL)]
        for k in range(1, nk):
            p, lb = mm_place(near_s[b, k - 1])
            mu = [wide(dyn[it][p, pl.ds(a * na + lb, 1), :]) for a in range(3)]
            for t in range(UNROLL):
                slot = ((i * UNROLL + t) * nk + k) * 4
                u = [geo[slot + a] for a in range(3)]
                cube = geo[slot + 3]
                proj = u[0] * mu[0] + u[1] * mu[1] + u[2] * mu[2]
                for a in range(3):
                    term = u[a] * proj - cube * mu[a]
                    acc[t][a] = acc[t][a] + term
        for k in range(nq):
            p, lb = grid_place(grid_s[b, k])
            q = wide(dyn[it][p, pl.ds(3 * na + lb, 1), :])
            for t in range(UNROLL):
                slot = ((i * UNROLL + t) * nq + k) * 3
                for a in range(3):
                    acc[t][a] = acc[t][a] + cgeo[slot + a] * q
        out = []
        for a in range(3):
            row = jnp.zeros((SUB, BLOCK), jnp.float32)
            for t in range(UNROLL):
                total = jnp.sum(acc[t][a], axis=1, keepdims=True)
                row = jnp.where(diag == (first + t) * SUB, total, row)
            out.append(row)
        for a in range(3):
            fld[i * 3 + a] = out[a]
        return carry

    def near_grid(it, i, carry):
        b = lax.div(i, HALVES)
        first = lax.rem(i, HALVES) * UNROLL
        acc = [None] * UNROLL
        for k in range(nm):
            p, lb = mm_place(source_s[b, k])
            mu = [wide(dyn[it][p, pl.ds(a * na + lb, 1), :]) for a in range(3)]
            for t in range(UNROLL):
                slot = ((i * UNROLL + t) * nm + k) * 3
                term = pgeo[slot] * mu[0] + pgeo[slot + 1] * mu[1] + pgeo[slot + 2] * mu[2]
                acc[t] = term if k == 0 else acc[t] + term
        row = jnp.zeros((SUB, BLOCK), jnp.float32)
        for t in range(UNROLL):
            total = jnp.sum(acc[t], axis=1, keepdims=True)
            row = jnp.where(diag == (first + t) * SUB, total, row)
        fld[na * HALVES * 3 + i] = row
        return carry

    def far_geometry(row_of):
        c = lax.broadcasted_iota(jnp.int32, (cells, BLOCK), 0)
        dx = row_of(0) - (c.astype(jnp.float32) + 0.5)
        dy = jnp.broadcast_to(row_of(1) - 0.5, (cells, BLOCK))
        dz = jnp.broadcast_to(row_of(2) - 0.5, (cells, BLOCK))
        inv = inverse_of(dx, dy, dz)
        cube = jnp.where(jnp.abs(c - cell) >= 2, inv * inv * inv, 0.0)
        return (dx, dy, dz), cube, cube * inv * inv * 3.0

    for_neighbours(stat, stat_send, stat_recv, start)
    for_peers(stat, stat_send, stat_recv, start)
    for_neighbours(dyn[0], dyn_send.at[0], dyn_recv.at[0], start)
    for_peers(dyn[0], dyn_send.at[0], dyn_recv.at[0], start)

    for it in range(ITERS):
        send, recv = dyn_send.at[it], dyn_recv.at[it]
        if it > 0:
            for_neighbours(dyn[it], send, recv, start)
            for_peers(dyn[it], send, recv, start)
        own_sums(it)
        each_other_cell(lambda c, g: far_copy(it, c, g).start())
        lax.fori_loop(0, na * HALVES, functools.partial(self_atoms, it), 0)
        if it == 0:
            peers_arrive(stat, stat_send, stat_recv)
            neighbours_arrive(stat, stat_send, stat_recv)
            lax.fori_loop(0, na * HALVES, geometry_atoms, 0)
            lax.fori_loop(0, ng * HALVES, geometry_grid, 0)
        peers_arrive(dyn[it], send, recv)
        neighbours_arrive(dyn[it], send, recv)
        lax.fori_loop(0, na * HALVES, functools.partial(near_atoms, it), 0)
        lax.fori_loop(0, ng * HALVES, functools.partial(near_grid, it), 0)
        far_all(it).wait_recv()
        sums = far_sums(it)
        moments = [sums[a] + sums[4 + a] for a in range(3)]
        for b in range(na):
            delta, cube, fifth = far_geometry(lambda a: vec_row(sites, a, b))
            radial = fifth * (moments[0] * delta[0] + moments[1] * delta[1] + moments[2] * delta[2])
            radial = radial + sums[3] * cube
            for a in range(3):
                far = column_sum(radial * delta[a] - moments[a] * cube)
                near = fld[b * HALVES * 3 + a]
                for h in range(1, HALVES):
                    near = near + fld[(b * HALVES + h) * 3 + a]
                new = flat_row(pol, b) * (vec_row(fixed, a, b) + (column_sum(near) + far))
                if it + 1 < ITERS:
                    dyn[it + 1][own, a * na + b : a * na + b + 1, :] = new
                else:
                    out_dip[a : a + 1, b * BLOCK : (b + 1) * BLOCK] = new
        for b in range(ng):
            delta, cube, _ = far_geometry(lambda a: vec_row(points, a, b))
            proj = sums[0] * delta[0] + sums[1] * delta[1] + sums[2] * delta[2]
            far = column_sum(proj * cube)
            slot = na * HALVES * 3 + b * HALVES
            near = fld[slot]
            for h in range(1, HALVES):
                near = near + fld[slot + h]
            new = flat_row(base, b) - flat_row(resp, b) * (column_sum(near) + far)
            if it + 1 < ITERS:
                dyn[it + 1][own, 3 * na + b : 3 * na + b + 1, :] = new
            else:
                out_q[b * BLOCK : (b + 1) * BLOCK] = new.reshape(BLOCK)

    def finish(copy):
        copy.wait_send()

    for_peers(stat, stat_send, stat_recv, finish)
    for_neighbours(stat, stat_send, stat_recv, finish)
    for it in range(ITERS):
        for_peers(dyn[it], dyn_send.at[it], dyn_recv.at[it], finish)
        for_neighbours(dyn[it], dyn_send.at[it], dyn_recv.at[it], finish)
        far_all(it).wait_send()


def solution(mesh):
    cells, grps = mesh.shape["cell"], mesh.shape["grp"]

    def step(sites, points, guess, fixed, pol, base, resp, near, grid, source):
        na, nb = near.shape
        nq = grid.shape[1]
        ng, nm = source.shape
        stat_rows = round_up(3 * na + 3 * ng, SUB)
        dyn_rows = round_up(3 * na + ng, SUB)
        f32 = jnp.float32
        args = (near, grid, source, sites, points, guess, fixed, pol, base, resp)
        vmem = pl.BlockSpec(memory_space=pltpu.VMEM)
        dma = pltpu.SemaphoreType.DMA
        return pl.pallas_call(
            functools.partial(body, (cells, grps, na, ng, nb, nq, nm)),
            out_shape=(
                jax.ShapeDtypeStruct(sites.shape, f32),
                jax.ShapeDtypeStruct(base.shape, f32),
            ),
            in_specs=[pl.BlockSpec(memory_space=pl.ANY)] * 10,
            out_specs=(vmem, vmem),
            scratch_shapes=[pltpu.SMEM(x.shape, x.dtype) for x in args[:3]]
            + [pltpu.VMEM(x.shape, x.dtype) for x in args[3:]]
            + [pltpu.VMEM((3 * grps, stat_rows, BLOCK), f32)]
            + [pltpu.VMEM((3 * grps, dyn_rows, BLOCK), f32) for _ in range(ITERS)]
            + [pltpu.VMEM((cells * grps, 1, BLOCK), f32) for _ in range(ITERS)]
            + [
                pltpu.VMEM((na, 3, BLOCK, BLOCK), f32),
                pltpu.VMEM((ng, 3, BLOCK, BLOCK), f32),
                pltpu.VMEM((na * GROUPS * (nb + 1) * 4, SUB, BLOCK), f32),
                pltpu.VMEM((na * GROUPS * nq * 3, SUB, BLOCK), f32),
                pltpu.VMEM((ng * GROUPS * nm * 3, SUB, BLOCK), f32),
                pltpu.VMEM(((na * 3 + ng) * HALVES, SUB, BLOCK), f32),
                pltpu.VMEM((na * GROUPS * 3, SUB, BLOCK), f32),
                dma((10,)),
                dma((3 * grps,)),
                dma((3 * grps,)),
                dma((ITERS, 3 * grps)),
                dma((ITERS, 3 * grps)),
                dma((ITERS,)),
                dma((ITERS,)),
            ],
            compiler_params=pltpu.CompilerParams(collective_id=0, has_side_effects=True),
        )(*args)

    pair = P(("cell", "grp"))
    wide = P(None, ("cell", "grp"))
    tall = P(("cell", "grp"), None)
    return jax.shard_map(
        step,
        mesh=mesh,
        in_specs=(wide, wide, wide, wide, pair, pair, pair, tall, tall, tall),
        out_specs=(wide, pair),
        check_vma=False,
    )
```
